32 devices in a mesh: types: 16 (over z, y, x), tm: 2 (over core).
Axes of the slice: x: 2, y: 2, z: 4, core: 2. Of those that a mesh axis runs over, the one named last changes fastest.
Arguments:
- brackets: int32 [96, 8, 7, 512], P('types', 'tm'), may hold values from 0 to 510, as said below
- active_blocks: int32 [96], P('types'), may hold values from 1 to 4, as said below
- initial_mass: float32 [96, 7, 512], P('types'), may hold values from 0 to 0.00055803574
- patience: float32 [96], P('types'), may hold values from 0.9 to 0.985
- productivity: float32 [96], P('types'), may hold values from 0.5 to 2
- income_levels: float32 [7], replicated, may hold values from 0.3 to 3
- income_transition: float32 [7, 7], replicated, may hold values from 0 to 1, as said below
- wage_path: float32 [8], replicated, may hold values from 0.8 to 1.2
- bond_supply: float32 [8], replicated, may hold values from 0.5 to 2
- price_guess: float32 [8], replicated, may hold values from -3 to 3
- jac_inverse: float32 [8, 8], replicated, may hold values from -2 to 2
- assignment: int32 [96], replicated, may hold values from 0 to 95, each once
Outputs:
- price_path: float32 [8], replicated
- market_gap: float32 [8], replicated
- type_paths: float32 [96, 2, 8], P('types')
The draws below stay inside these ranges and needn't reach their ends.
Inputs may be any that keep to these rules, and one draw needn't show every extreme that they name: `brackets`: the bracket of asset point i lies between max(i - 9, 0) and max(i - 1, 0). `active_blocks`: counts of 128-point blocks from the bottom of the grid. `income_transition`: rows of positive entries summing to one. `assignment`: each type appears once.
All inputs are finite; a program needn't handle non-finite values.
Results may differ from the reference program's by a relative error of at most 0.0003.
Values sent between devices are 32-bit elements; how exact they have to be, the bound alone decides.
A program may use at most 64 MiB of HBM per device.

```python
import math
import jax
import jax.numpy as jnp
from jax import lax

ASSETS = 512
INCOME = 7
BLOCK = 128
REACH = 8
NEWTON = 2
TYPES_DEV = 6
TYPES = 96
PERIODS = 8


def draw_brackets(key, part):
    points = jnp.arange(ASSETS, dtype=jnp.int32)
    drop_sizes = jax.random.randint(key, (TYPES, PERIODS, INCOME, ASSETS), 0, REACH + 1)
    return jnp.maximum(points - 1 - drop_sizes, 0).astype(jnp.int32)


def draw_active_blocks(key, part):
    largest = ASSETS // BLOCK
    groups = TYPES // TYPES_DEV
    heavy_key = jax.random.fold_in(key, 11)
    pick_key = jax.random.fold_in(key, 12)
    jitter_key = jax.random.fold_in(key, 13)
    full_key = jax.random.fold_in(key, 14)
    heavy_group = jax.random.randint(heavy_key, (groups,), 0, 4) == 0
    heavy_group = heavy_group.at[jax.random.randint(pick_key, (), 0, groups)].set(True)
    heavy_rows = jnp.repeat(heavy_group, TYPES_DEV)
    jitter = jax.random.randint(jitter_key, (TYPES,), 0, 2)
    counts = jnp.where(heavy_rows, largest - 1 + jitter, 1 + jitter)
    counts = counts.at[jax.random.randint(full_key, (), 0, TYPES)].set(largest)
    return counts.astype(jnp.int32)


def draw_income_transition(key, part):
    raw_values = jax.random.uniform(key, (INCOME, INCOME), jnp.float32, 0.2, 1.0) + 2.0 * jnp.eye(INCOME, dtype=jnp.float32)
    return raw_values / jnp.sum(raw_values, axis=1, keepdims=True)


def level_of(key, shape, split, smallest, top_value):
    level = 1.0
    for axis_at, blocks in split:
        heights = jax.random.uniform(jax.random.fold_in(jax.random.fold_in(key, 6), axis_at), (blocks,), jnp.float32, smallest / len(split), top_value / len(split))
        level = level * jnp.repeat(jnp.exp(heights), shape[axis_at] // blocks).reshape((-1,) + (1,) * (len(shape) - 1 - axis_at))
    return level


def centred(own_key, dims, scale, bound, kind=jnp.bfloat16):
    entries = scale * jax.random.normal(own_key, dims, jnp.float32)
    return jnp.clip(entries, min=-bound, max=bound).astype(kind)


def setup_inputs(seed: int = 0) -> dict:
    keys = jax.random.split(jax.random.key(seed), 13)
    return {
        "brackets": draw_brackets(jax.random.fold_in(keys[12], 71), 0),
        "active_blocks": draw_active_blocks(jax.random.fold_in(keys[12], 71), 0),
        "initial_mass": jnp.clip(0.00055803574 * jax.random.uniform(keys[2], (TYPES, INCOME, ASSETS), jnp.float32) ** level_of(keys[2], (TYPES, INCOME, ASSETS), ((0, 16),), -0.2, 0.2), 0.0, 0.00055803574),
        "patience": jnp.clip(0.9 + 0.08500004 * jax.random.uniform(keys[3], (TYPES,), jnp.float32) ** level_of(keys[3], (TYPES,), ((0, 16),), -0.2, 0.2), 0.9, 0.985),
        "productivity": jnp.clip(jnp.exp(math.log(2.0) - 1.3862944 * jax.random.uniform(keys[4], (TYPES,), jnp.float32) ** level_of(keys[4], (TYPES,), ((0, 16),), -0.2, 0.2)), 0.5, 2.0),
        "income_levels": jnp.clip(jnp.exp(jax.random.uniform(keys[5], (INCOME,), jnp.float32, math.log(0.3), math.log(3.0))), 0.3, 3.0),
        "income_transition": draw_income_transition(jax.random.fold_in(keys[12], 71), 0),
        "wage_path": jnp.clip(jax.random.uniform(keys[7], (PERIODS,), jnp.float32, 0.8, 1.2), 0.8, 1.2),
        "bond_supply": jnp.clip(jax.random.uniform(keys[8], (PERIODS,), jnp.float32, 0.5, 2.0), 0.5, 2.0),
        "price_guess": centred(keys[9], (PERIODS,), 1.0, 3.0, jnp.float32),
        "jac_inverse": centred(keys[10], (PERIODS, PERIODS), PERIODS ** -0.5, 2.0, jnp.float32),
        "assignment": jax.random.permutation(keys[11], TYPES).astype(jnp.int32),
    }


grid_top = 40.0
rate_floor = 0.005
rate_span = 0.03
highest = lax.Precision.HIGHEST


def asset_grid(points):
    return grid_top * (points / (ASSETS - 1)) ** 2


def interest(price_path):
    return rate_floor + rate_span * jax.nn.sigmoid(price_path)


def policy(lower_edge, upper_edge, bracket_now, rate_now, income_now, grid_rows):
    grid_low = asset_grid(bracket_now.astype(jnp.float32))
    grid_high = asset_grid((bracket_now + 1).astype(jnp.float32))
    spacing = jnp.maximum(upper_edge - lower_edge, (grid_high - grid_low) / (1.0 + rate_now))
    weight_up = jnp.clip((grid_rows[None, :] - lower_edge) / spacing, 0.0, 1.0)
    savings = grid_low + weight_up * (grid_high - grid_low)
    spending = (1.0 + rate_now) * grid_rows[None, :] + income_now[:, None] - savings
    return weight_up, savings, spending


def solve_type(bracket, mass_start, blocks, patience, productivity, interest_path, wage_path, income_levels, transition):
    grid_values = asset_grid(jnp.arange(ASSETS, dtype=jnp.float32))
    incomes = wage_path[:, None] * productivity * income_levels[None, :]
    last_rate = interest_path[-1]
    values_end = (1.0 + last_rate) / (last_rate * grid_values[None, :] + incomes[-1][:, None])

    def backward(values, inputs):
        bracket_now, rate_now, income_now = inputs
        expected = patience * jnp.dot(transition, values, precision=highest)
        endogenous = (1.0 / expected + grid_values[None, :] - income_now[:, None]) / (1.0 + rate_now)
        lower_edge = jnp.take_along_axis(endogenous, bracket_now, axis=1)
        upper_edge = jnp.take_along_axis(endogenous, bracket_now + 1, axis=1)
        weight_up, savings, spending = policy(lower_edge, upper_edge, bracket_now, rate_now, income_now, grid_values)
        return (1.0 + rate_now) / spending, (weight_up, savings, spending)

    values_start, policies = lax.scan(backward, values_end, (bracket, interest_path, incomes), reverse=True)
    live_rows = (jnp.arange(ASSETS, dtype=jnp.int32) < blocks * BLOCK).astype(jnp.float32)
    masses = mass_start * live_rows[None, :]

    def spread(target_row, staying, rising):
        empty = jnp.zeros((ASSETS,), jnp.float32)
        return empty.at[target_row].add(staying).at[target_row + 1].add(rising)

    def forward(masses, inputs):
        bracket_now, weight_up, savings, spending = inputs
        totals = jnp.stack([jnp.sum(masses * savings), jnp.sum(masses * spending)])
        arrived = jax.vmap(spread)(bracket_now, (1.0 - weight_up) * masses, weight_up * masses)
        return jnp.dot(transition.T, arrived, precision=highest), totals

    masses_end, type_series = lax.scan(forward, masses, (bracket, policies[0], policies[1], policies[2]))
    return type_series.T


def reference(brackets, active_blocks, initial_mass, patience, productivity, income_levels, income_transition, wage_path, bond_supply, price_guess, jac_inverse, assignment):
    price_path = price_guess
    market_gap = jnp.zeros_like(price_guess)
    type_series = jnp.zeros((TYPES, 2, PERIODS), jnp.float32)
    for newton_round in range(NEWTON):
        interest_path = interest(price_path)

        def solve_member(members):
            return solve_type(members[0], members[1], members[2], members[3], members[4], interest_path, wage_path, income_levels, income_transition)

        type_series = lax.map(solve_member, (brackets, initial_mass, active_blocks, patience, productivity))
        totals = jnp.sum(type_series[:, 0, :], axis=0)
        market_gap = totals / TYPES - bond_supply
        price_path = price_path - jnp.dot(jac_inverse, market_gap, precision=highest)
    type_paths = type_series[assignment]
    return price_path, market_gap, type_paths
```

```python
import functools

import jax
import jax.numpy as jnp
from jax import lax
from jax.experimental import pallas as pl
from jax.experimental.pallas import tpu as pltpu
from jax.sharding import PartitionSpec as P

BLOCK = 128
REACH = 8
NEWTON = 2
ROWS = 8
LANES = 128

grid_top = 40.0
rate_floor = 0.005
rate_span = 0.03
MESH = pl.DeviceIdType.MESH


def iota(axis):
    return lax.broadcasted_iota(jnp.int32, (ROWS, LANES), axis)


def take(source, index):
    return jnp.take_along_axis(source, index, axis=1, mode="promise_in_bounds")


def to_column(row):
    spread = jnp.where(iota(0) == iota(1), jnp.broadcast_to(row, (ROWS, LANES)), 0.0)
    return jnp.sum(spread, axis=1, keepdims=True)


def to_row(column, offset):
    spread = jnp.where(iota(0) + offset == iota(1), jnp.broadcast_to(column, (ROWS, LANES)), 0.0)
    return jnp.sum(spread, axis=0, keepdims=True)


def shifted(row, lanes):
    return row if lanes == 0 else pltpu.roll(row, LANES - lanes, 1)


def kernel(
    sizes,
    brackets, active, initial_mass, patience, productivity, levels, transition,
    wage, bond, price_in, jac, assignment,
    price_out, gap_out, paths_out,
    br, mass_in, vals, mass, arrived, weights, savings, spending, totals,
    t_back, t_fwd, level_col, rates, send_row, recv_a, recv_b,
    br_sem, br_send, mass_sem, row_send, row_recv,
):
    groups, cores, local_types, periods, incomes, assets = sizes
    mine = local_types // cores
    here = periods // cores
    blocks = assets // LANES
    devices = groups * cores
    group = lax.axis_index("types")
    core = lax.axis_index("tm")
    me = group * cores + core
    grid_unit = grid_top / float(assets - 1) ** 2

    def place(flat):
        return (flat // cores, lax.rem(flat, cores))

    def local_copy(p):
        return pltpu.make_async_copy(
            brackets.at[pl.ds(core * mine, mine), p],
            br.at[core * here + p],
            br_sem.at[core * here + p],
        )

    for p in reversed(range(here)):
        local_copy(p).start()
    mass_copy = pltpu.make_async_copy(
        initial_mass.at[pl.ds(core * mine, mine)],
        mass_in,
        mass_sem.at[0],
    )
    mass_copy.start()

    barrier = pltpu.get_barrier_semaphore()

    def greet(o, carry):
        pl.semaphore_signal(
            barrier, inc=1, device_id=place(lax.rem(me + o, devices)), device_id_type=MESH
        )
        return carry

    lax.fori_loop(1, devices, greet, 0)

    row_id = iota(0)
    lane_id = iota(1)
    for f in range(incomes):
        back = jnp.full((ROWS, LANES), 1.0 / incomes, jnp.float32)
        ahead = jnp.zeros((ROWS, LANES), jnp.float32)
        for e in range(incomes):
            back = jnp.where(row_id == e, transition[e, f], back)
            ahead = jnp.where(row_id == e, transition[f, e], ahead)
        t_back[f] = back
        t_fwd[f] = ahead
    column = jnp.ones((ROWS, LANES), jnp.float32)
    for e in range(incomes):
        column = jnp.where(row_id == e, levels[e], column)
    level_col[...] = column

    pl.semaphore_wait(barrier, devices - 1)

    def peer_copy(o, p):
        peer = lax.rem(core + o, cores)
        return pltpu.make_async_remote_copy(
            src_ref=brackets.at[pl.ds(peer * mine, mine), p],
            dst_ref=br.at[core * here + p],
            send_sem=br_send.at[o - 1, p],
            recv_sem=br_sem.at[core * here + p],
            device_id=(group, peer),
            device_id_type=MESH,
        )

    for p in reversed(range(here)):
        for o in range(1, cores):
            peer_copy(o, p).start()

    def grid_block(b):
        point = (lane_id + b * LANES).astype(jnp.float32)
        return grid_unit * (point * point)

    def full_rows(x):
        return jnp.pad(x, ((0, ROWS - incomes), (0, 0)))

    def lanes(b):
        return pl.ds(b * LANES, LANES)

    def bracket_block(t, k, b):
        return full_rows(br[t, k, :, lanes(b)])

    price = jnp.pad(price_in[...], ((0, 0), (0, LANES - periods)))
    bond_row = jnp.pad(bond[...], ((0, 0), (0, LANES - periods)))
    mass_copy.wait()

    for newton_round in range(NEWTON):
        last = newton_round + 1 == NEWTON
        rate_row = rate_floor + rate_span / (1.0 + jnp.exp(-price))
        rate_col = jnp.broadcast_to(to_column(rate_row), (ROWS, LANES))
        rates[0] = 1.0 + rate_col
        rates[1] = 1.0 / (1.0 + rate_col)
        end_gross = jnp.broadcast_to(rates[0, pl.ds(periods - 1, 1), :], (ROWS, LANES))
        end_rate = jnp.broadcast_to(rate_col[periods - 1 : periods, :], (ROWS, LANES))
        for k in range(mine):
            income = (wage[periods - 1] * productivity[core * mine + k]) * level_col[...]
            for b in range(blocks):
                vals[k, :, lanes(b)] = end_gross / (end_rate * grid_block(b) + income)
            live = active[core * mine + k] * BLOCK
            for b in range(blocks):
                start = full_rows(mass_in[k, :, lanes(b)])
                mass[k, :, lanes(b)] = jnp.where(lane_id + b * LANES < live, start, 0.0)

        def backward(step, carry):
            t = periods - 1 - step
            if newton_round == 0:
                pltpu.make_async_copy(
                    brackets.at[pl.ds(0, mine), 0],
                    br.at[t],
                    br_sem.at[t],
                ).wait()
            gross = jnp.broadcast_to(rates[0, pl.ds(t, 1), :], (ROWS, LANES))
            inverse = jnp.broadcast_to(rates[1, pl.ds(t, 1), :], (ROWS, LANES))
            for k in range(mine):
                income = (wage[t] * productivity[core * mine + k]) * level_col[...]
                patient = patience[core * mine + k]
                endogenous = []
                for b in range(blocks):
                    expected = None
                    for f in range(incomes):
                        term = t_back[f] * jnp.broadcast_to(
                            vals[k, pl.ds(f, 1), lanes(b)], (ROWS, LANES)
                        )
                        expected = term if expected is None else expected + term
                    endogenous.append(
                        (1.0 / (patient * expected) + grid_block(b) - income) * inverse
                    )
                for b in range(blocks):
                    j = bracket_block(t, k, b)
                    low_at = jnp.bitwise_and(j, LANES - 1)
                    high_at = jnp.bitwise_and(j + 1, LANES - 1)
                    lower = take(endogenous[b], low_at)
                    upper = take(endogenous[b], high_at)
                    if b > 0:
                        lower = jnp.where(j >= b * LANES, lower, take(endogenous[b - 1], low_at))
                        upper = jnp.where(
                            j + 1 >= b * LANES, upper, take(endogenous[b - 1], high_at)
                        )
                    jf = j.astype(jnp.float32)
                    grid_low = grid_unit * (jf * jf)
                    grid_step = grid_unit * (2.0 * jf + 1.0)
                    grid_here = grid_block(b)
                    spacing = jnp.maximum(upper - lower, grid_step * inverse)
                    weight = jnp.clip((grid_here - lower) / spacing, 0.0, 1.0)
                    saved = grid_low + weight * grid_step
                    spent = gross * grid_here + income - saved
                    weights[t, k, :, lanes(b)] = weight
                    savings[t, k, :, lanes(b)] = saved
                    if last:
                        spending[t, k, :, lanes(b)] = spent
                    vals[k, :, lanes(b)] = gross / spent
            return carry

        lax.fori_loop(0, periods, backward, 0)

        def forward(t, carry):
            for k in range(mine):
                assets_sum = None
                spent_sum = None
                stay, rise, drop = [], [], []
                for b in range(blocks):
                    now = mass[k, :, lanes(b)]
                    held = now * savings[t, k, :, lanes(b)]
                    assets_sum = held if assets_sum is None else assets_sum + held
                    if last:
                        used = now * spending[t, k, :, lanes(b)]
                        spent_sum = used if spent_sum is None else spent_sum + used
                    up = weights[t, k, :, lanes(b)] * now
                    rise.append(up)
                    stay.append(now - up)
                    drop.append(lane_id + b * LANES - bracket_block(t, k, b))
                totals[2 * k, t] = assets_sum
                if last:
                    totals[2 * k + 1, t] = spent_sum
                sums = [None] * blocks
                sums[0] = pltpu.roll(jnp.where(drop[0] == 0, rise[0], 0.0), 1, 1)
                for s in range(REACH + 2):
                    part = [
                        jnp.where(
                            drop[b] == s, stay[b], jnp.where(drop[b] == s + 1, rise[b], 0.0)
                        )
                        for b in range(blocks)
                    ]
                    for b in range(blocks):
                        piece = part[b]
                        if s > 0:
                            above = part[b + 1] if b + 1 < blocks else jnp.zeros_like(piece)
                            piece = shifted(jnp.where(lane_id >= s, piece, above), s)
                        sums[b] = piece if sums[b] is None else sums[b] + piece
                for b in range(blocks):
                    arrived[k, :, lanes(b)] = sums[b]
                for b in range(blocks):
                    new = None
                    for e in range(incomes):
                        term = t_fwd[e] * jnp.broadcast_to(
                            arrived[k, pl.ds(e, 1), lanes(b)], (ROWS, LANES)
                        )
                        new = term if new is None else new + term
                    mass[k, :, lanes(b)] = new
            return carry

        lax.fori_loop(0, periods, forward, 0)

        row = jnp.zeros((1, LANES), jnp.float32)
        if last:
            for c in range(2 * mine):
                series = jnp.sum(totals[c], axis=1)
                row = row + to_row(jnp.sum(series, axis=1, keepdims=True), c * periods)
        else:
            series = totals[0]
            for k in range(1, mine):
                series = series + totals[2 * k]
            series = jnp.sum(series, axis=1)
            row = to_row(jnp.sum(series, axis=1, keepdims=True), 0)
        inbox = recv_b if last else recv_a
        send_row[newton_round] = row
        inbox[me] = row

        def row_copy(o):
            return pltpu.make_async_remote_copy(
                src_ref=send_row.at[newton_round],
                dst_ref=inbox.at[me],
                send_sem=row_send.at[newton_round],
                recv_sem=row_recv.at[newton_round],
                device_id=place(lax.rem(me + o, devices)),
                device_id_type=MESH,
            )

        def send(o, carry):
            row_copy(o).start()
            return carry

        lax.fori_loop(1, devices, send, 0)
        others = inbox.at[pl.ds(0, devices - 1)]
        pltpu.make_async_copy(others, others, row_recv.at[newton_round]).wait()
        total = jnp.sum(inbox[0:devices], axis=0)
        if last:
            total = functools.reduce(
                jnp.add, [shifted(total, 2 * k * periods) for k in range(mine)]
            )
        gap = jnp.where(
            lane_id[0:1] < periods, total / float(groups * local_types) - bond_row, 0.0
        )
        change = jnp.sum(
            jac[...] * jnp.broadcast_to(gap[:, 0:periods], (periods, periods)),
            axis=1,
            keepdims=True,
        )
        price = price - to_row(change, 0)
        pltpu.make_async_copy(others, others, row_send.at[newton_round]).wait()

    price_out[...] = price[:, 0:periods]
    gap_out[...] = gap[:, 0:periods]
    for s in range(local_types):
        wanted = assignment[group * local_types + s]
        source = recv_b[wanted // mine]
        within = lax.rem(wanted, mine)
        found = source
        for k in range(1, mine):
            found = jnp.where(within == k, shifted(source, 2 * k * periods), found)
        paths_out[s, 0:1, :] = found[:, 0:periods]
        paths_out[s, 1:2, :] = shifted(found, periods)[:, 0:periods]

    for p in range(here):
        for o in range(1, cores):
            peer_copy(o, p).wait_send()


def body(groups, cores, *args):
    brackets, assignment = args[0], args[-1]
    local_types, here, incomes, assets = brackets.shape
    periods = here * cores
    mine = local_types // cores
    devices = groups * cores
    sizes = (groups, cores, local_types, periods, incomes, assets)
    assert 2 * mine * periods <= LANES and periods == ROWS and incomes <= ROWS
    args = list(args)
    args[8] = args[8].reshape(1, periods)
    args[9] = args[9].reshape(1, periods)
    vmem = pl.BlockSpec(memory_space=pltpu.VMEM)
    smem = pl.BlockSpec(memory_space=pltpu.SMEM)
    far = pl.BlockSpec(memory_space=pl.ANY)
    f32 = jnp.float32
    per_period = pltpu.VMEM((periods, mine, ROWS, assets), f32)
    per_type = pltpu.VMEM((mine + 1, ROWS, assets), f32)
    price, gap, paths = pl.pallas_call(
        functools.partial(kernel, sizes),
        out_shape=(
            jax.ShapeDtypeStruct((1, periods), f32),
            jax.ShapeDtypeStruct((1, periods), f32),
            jax.ShapeDtypeStruct((local_types, 2, periods), f32),
        ),
        in_specs=[far, smem, far, smem, smem, smem, smem, smem, vmem, vmem, vmem, smem],
        out_specs=(vmem, vmem, vmem),
        scratch_shapes=[
            pltpu.VMEM((periods, mine, incomes, assets), jnp.int32),
            pltpu.VMEM((mine, incomes, assets), f32),
            per_type, per_type, per_type,
            per_period, per_period, per_period,
            pltpu.VMEM((2 * mine, periods, ROWS, LANES), f32),
            pltpu.VMEM((incomes, ROWS, LANES), f32),
            pltpu.VMEM((incomes, ROWS, LANES), f32),
            pltpu.VMEM((ROWS, LANES), f32),
            pltpu.VMEM((3, ROWS, LANES), f32),
            pltpu.VMEM((NEWTON + ROWS, 1, LANES), f32),
            pltpu.VMEM((devices + ROWS, 1, LANES), f32),
            pltpu.VMEM((devices + ROWS, 1, LANES), f32),
            pltpu.SemaphoreType.DMA((periods,)),
            pltpu.SemaphoreType.DMA((cores - 1, here)),
            pltpu.SemaphoreType.DMA((1,)),
            pltpu.SemaphoreType.DMA((NEWTON,)),
            pltpu.SemaphoreType.DMA((NEWTON,)),
        ],
        compiler_params=pltpu.CompilerParams(collective_id=0, has_side_effects=True),
    )(*args)
    return price.reshape(periods), gap.reshape(periods), paths


def solution(mesh):
    placed = (
        P("types", "tm", None, None),
        P("types"),
        P("types", None, None),
        P("types"),
        P("types"),
        P(),
        P(),
        P(),
        P(),
        P(),
        P(),
        P(),
    )
    return jax.shard_map(
        functools.partial(body, mesh.shape["types"], mesh.shape["tm"]),
        mesh=mesh,
        in_specs=placed,
        out_specs=(P(), P(), P("types", None, None)),
        check_vma=False,
    )
```

```python
import functools

import jax
import jax.numpy as jnp
from jax import lax
from jax.experimental import pallas as pl
from jax.experimental.pallas import tpu as pltpu
from jax.sharding import PartitionSpec as P

BLOCK = 128
REACH = 8
NEWTON = 2
ROWS = 8
LANES = 128

grid_top = 40.0
rate_floor = 0.005
rate_span = 0.03
MESH = pl.DeviceIdType.MESH


def iota(axis):
    return lax.broadcasted_iota(jnp.int32, (ROWS, LANES), axis)


def take(source, index):
    return jnp.take_along_axis(source, index, axis=1, mode="promise_in_bounds")


def to_column(row):
    spread = jnp.where(iota(0) == iota(1), jnp.broadcast_to(row, (ROWS, LANES)), 0.0)
    return jnp.sum(spread, axis=1, keepdims=True)


def to_row(column, offset):
    spread = jnp.where(iota(0) + offset == iota(1), jnp.broadcast_to(column, (ROWS, LANES)), 0.0)
    return jnp.sum(spread, axis=0, keepdims=True)


def shifted(row, lanes):
    return row if lanes == 0 else pltpu.roll(row, LANES - lanes, 1)


def kernel(
    sizes,
    brackets, active, initial_mass, patience, productivity, levels, transition,
    wage, bond, price_in, jac, assignment,
    price_out, gap_out, paths_out,
    br, mass_in, vals, mass, arrived, weights, savings, spending, totals,
    t_back, t_fwd, level_col, rates, send_row, recv_a, recv_b,
    br_sem, br_send, mass_sem, row_send, row_recv,
):
    groups, cores, local_types, periods, incomes, assets = sizes
    mine = local_types // cores
    here = periods // cores
    blocks = assets // LANES
    devices = groups * cores
    group = lax.axis_index("types")
    core = lax.axis_index("tm")
    me = group * cores + core
    grid_unit = grid_top / float(assets - 1) ** 2

    def place(flat):
        return (flat // cores, lax.rem(flat, cores))

    def local_copy(p):
        return pltpu.make_async_copy(
            brackets.at[pl.ds(core * mine, mine), :, p],
            br.at[core * here + p],
            br_sem.at[core * here + p],
        )

    for p in reversed(range(here)):
        local_copy(p).start()
    mass_copy = pltpu.make_async_copy(
        initial_mass.at[pl.ds(core * mine, mine)],
        mass_in,
        mass_sem.at[0],
    )
    mass_copy.start()

    barrier = pltpu.get_barrier_semaphore()

    def greet(o, carry):
        pl.semaphore_signal(
            barrier, inc=1, device_id=place(lax.rem(me + o, devices)), device_id_type=MESH
        )
        return carry

    lax.fori_loop(1, devices, greet, 0)

    row_id = iota(0)
    lane_id = iota(1)
    for f in range(incomes):
        back = jnp.full((ROWS, LANES), 1.0 / incomes, jnp.float32)
        ahead = jnp.zeros((ROWS, LANES), jnp.float32)
        for e in range(incomes):
            back = jnp.where(row_id == e, transition[e, f], back)
            ahead = jnp.where(row_id == e, transition[f, e], ahead)
        t_back[f] = back
        t_fwd[f] = ahead
    column = jnp.ones((ROWS, LANES), jnp.float32)
    for e in range(incomes):
        column = jnp.where(row_id == e, levels[e], column)
    level_col[...] = column

    pl.semaphore_wait(barrier, devices - 1)

    def peer_copy(o, p):
        peer = lax.rem(core + o, cores)
        return pltpu.make_async_remote_copy(
            src_ref=brackets.at[pl.ds(peer * mine, mine), :, p],
            dst_ref=br.at[core * here + p],
            send_sem=br_send.at[o - 1, p],
            recv_sem=br_sem.at[core * here + p],
            device_id=(group, peer),
            device_id_type=MESH,
        )

    for p in reversed(range(here)):
        for o in range(1, cores):
            peer_copy(o, p).start()

    def grid_block(b):
        point = (lane_id + b * LANES).astype(jnp.float32)
        return grid_unit * (point * point)

    def full_rows(x):
        return jnp.pad(x, ((0, ROWS - incomes), (0, 0)))

    def lanes(b):
        return pl.ds(b * LANES, LANES)

    def bracket_block(t, k, b):
        return full_rows(br[t, k, :, lanes(b)])

    price = jnp.pad(price_in[...], ((0, 0), (0, LANES - periods)))
    bond_row = jnp.pad(bond[...], ((0, 0), (0, LANES - periods)))
    mass_copy.wait()

    for newton_round in range(NEWTON):
        last = newton_round + 1 == NEWTON
        rate_row = rate_floor + rate_span / (1.0 + jnp.exp(-price))
        rate_col = jnp.broadcast_to(to_column(rate_row), (ROWS, LANES))
        rates[0] = 1.0 + rate_col
        rates[1] = 1.0 / (1.0 + rate_col)
        end_gross = jnp.broadcast_to(rates[0, pl.ds(periods - 1, 1), :], (ROWS, LANES))
        end_rate = jnp.broadcast_to(rate_col[periods - 1 : periods, :], (ROWS, LANES))
        for k in range(mine):
            income = (wage[periods - 1] * productivity[core * mine + k]) * level_col[...]
            for b in range(blocks):
                vals[k, :, lanes(b)] = end_gross / (end_rate * grid_block(b) + income)
            live = active[core * mine + k] * BLOCK
            for b in range(blocks):
                start = full_rows(mass_in[k, :, lanes(b)])
                mass[k, :, lanes(b)] = jnp.where(lane_id + b * LANES < live, start, 0.0)

        def backward(step, carry):
            t = periods - 1 - step
            if newton_round == 0:
                pltpu.make_async_copy(
                    brackets.at[pl.ds(0, mine), :, 0],
                    br.at[t],
                    br_sem.at[t],
                ).wait()
            gross = jnp.broadcast_to(rates[0, pl.ds(t, 1), :], (ROWS, LANES))
            inverse = jnp.broadcast_to(rates[1, pl.ds(t, 1), :], (ROWS, LANES))
            for k in range(mine):
                income = (wage[t] * productivity[core * mine + k]) * level_col[...]
                patient = patience[core * mine + k]
                endogenous = []
                for b in range(blocks):
                    expected = None
                    for f in range(incomes):
                        term = t_back[f] * jnp.broadcast_to(
                            vals[k, pl.ds(f, 1), lanes(b)], (ROWS, LANES)
                        )
                        expected = term if expected is None else expected + term
                    endogenous.append(
                        (1.0 / (patient * expected) + grid_block(b) - income) * inverse
                    )
                for b in range(blocks):
                    j = bracket_block(t, k, b)
                    low_at = jnp.bitwise_and(j, LANES - 1)
                    high_at = jnp.bitwise_and(j + 1, LANES - 1)
                    lower = take(endogenous[b], low_at)
                    upper = take(endogenous[b], high_at)
                    if b > 0:
                        lower = jnp.where(j >= b * LANES, lower, take(endogenous[b - 1], low_at))
                        upper = jnp.where(
                            j + 1 >= b * LANES, upper, take(endogenous[b - 1], high_at)
                        )
                    jf = j.astype(jnp.float32)
                    grid_low = grid_unit * (jf * jf)
                    grid_step = grid_unit * (2.0 * jf + 1.0)
                    grid_here = grid_block(b)
                    spacing = jnp.maximum(upper - lower, grid_step * inverse)
                    weight = jnp.clip((grid_here - lower) / spacing, 0.0, 1.0)
                    saved = grid_low + weight * grid_step
                    spent = gross * grid_here + income - saved
                    weights[t, k, :, lanes(b)] = weight
                    savings[t, k, :, lanes(b)] = saved
                    if last:
                        spending[t, k, :, lanes(b)] = spent
                    vals[k, :, lanes(b)] = gross / spent
            return carry

        lax.fori_loop(0, periods, backward, 0)

        def forward(t, carry):
            for k in range(mine):
                assets_sum = None
                spent_sum = None
                stay, rise, drop = [], [], []
                for b in range(blocks):
                    now = mass[k, :, lanes(b)]
                    held = now * savings[t, k, :, lanes(b)]
                    assets_sum = held if assets_sum is None else assets_sum + held
                    if last:
                        used = now * spending[t, k, :, lanes(b)]
                        spent_sum = used if spent_sum is None else spent_sum + used
                    up = weights[t, k, :, lanes(b)] * now
                    rise.append(up)
                    stay.append(now - up)
                    drop.append(lane_id + b * LANES - bracket_block(t, k, b))
                totals[2 * k, t] = assets_sum
                if last:
                    totals[2 * k + 1, t] = spent_sum
                sums = [None] * blocks
                sums[0] = pltpu.roll(jnp.where(drop[0] == 0, rise[0], 0.0), 1, 1)
                for s in range(REACH + 2):
                    part = [
                        jnp.where(
                            drop[b] == s, stay[b], jnp.where(drop[b] == s + 1, rise[b], 0.0)
                        )
                        for b in range(blocks)
                    ]
                    for b in range(blocks):
                        piece = part[b]
                        if s > 0:
                            above = part[b + 1] if b + 1 < blocks else jnp.zeros_like(piece)
                            piece = shifted(jnp.where(lane_id >= s, piece, above), s)
                        sums[b] = piece if sums[b] is None else sums[b] + piece
                for b in range(blocks):
                    arrived[k, :, lanes(b)] = sums[b]
                for b in range(blocks):
                    new = None
                    for e in range(incomes):
                        term = t_fwd[e] * jnp.broadcast_to(
                            arrived[k, pl.ds(e, 1), lanes(b)], (ROWS, LANES)
                        )
                        new = term if new is None else new + term
                    mass[k, :, lanes(b)] = new
            return carry

        lax.fori_loop(0, periods, forward, 0)

        row = jnp.zeros((1, LANES), jnp.float32)
        if last:
            for c in range(2 * mine):
                series = jnp.sum(totals[c], axis=1)
                row = row + to_row(jnp.sum(series, axis=1, keepdims=True), c * periods)
        else:
            series = totals[0]
            for k in range(1, mine):
                series = series + totals[2 * k]
            series = jnp.sum(series, axis=1)
            row = to_row(jnp.sum(series, axis=1, keepdims=True), 0)
        inbox = recv_b if last else recv_a
        send_row[newton_round] = row
        inbox[me] = row

        def row_copy(o):
            return pltpu.make_async_remote_copy(
                src_ref=send_row.at[newton_round],
                dst_ref=inbox.at[me],
                send_sem=row_send.at[newton_round],
                recv_sem=row_recv.at[newton_round],
                device_id=place(lax.rem(me + o, devices)),
                device_id_type=MESH,
            )

        def send(o, carry):
            row_copy(o).start()
            return carry

        lax.fori_loop(1, devices, send, 0)
        others = inbox.at[pl.ds(0, devices - 1)]
        pltpu.make_async_copy(others, others, row_recv.at[newton_round]).wait()
        total = jnp.sum(inbox[0:devices], axis=0)
        if last:
            total = functools.reduce(
                jnp.add, [shifted(total, 2 * k * periods) for k in range(mine)]
            )
        gap = jnp.where(
            lane_id[0:1] < periods, total / float(groups * local_types) - bond_row, 0.0
        )
        change = jnp.sum(
            jac[...] * jnp.broadcast_to(gap[:, 0:periods], (periods, periods)),
            axis=1,
            keepdims=True,
        )
        price = price - to_row(change, 0)
        pltpu.make_async_copy(others, others, row_send.at[newton_round]).wait()

    price_out[...] = price[:, 0:periods]
    gap_out[...] = gap[:, 0:periods]
    for s in range(local_types):
        wanted = assignment[group * local_types + s]
        source = recv_b[wanted // mine]
        within = lax.rem(wanted, mine)
        found = source
        for k in range(1, mine):
            found = jnp.where(within == k, shifted(source, 2 * k * periods), found)
        paths_out[s, 0:1, :] = found[:, 0:periods]
        paths_out[s, 1:2, :] = shifted(found, periods)[:, 0:periods]

    for p in range(here):
        for o in range(1, cores):
            peer_copy(o, p).wait_send()


def hand_out(price, gap, paths, price_out, gap_out, paths_out):
    price_out[...] = price[...]
    gap_out[...] = gap[...]
    paths_out[...] = paths[...]


def body(groups, cores, *args):
    brackets, assignment = args[0], args[-1]
    local_types, here, incomes, assets = brackets.shape
    periods = here * cores
    mine = local_types // cores
    devices = groups * cores
    sizes = (groups, cores, local_types, periods, incomes, assets)
    assert 2 * mine * periods <= LANES and periods == ROWS and incomes <= ROWS
    args = list(args)
    args[0] = jnp.transpose(brackets, (0, 2, 1, 3))
    args[8] = args[8].reshape(1, periods)
    args[9] = args[9].reshape(1, periods)
    vmem = pl.BlockSpec(memory_space=pltpu.VMEM)
    smem = pl.BlockSpec(memory_space=pltpu.SMEM)
    far = pl.BlockSpec(memory_space=pl.ANY)
    f32 = jnp.float32
    per_period = pltpu.VMEM((periods, mine, ROWS, assets), f32)
    per_type = pltpu.VMEM((mine + 1, ROWS, assets), f32)
    price, gap, paths = pl.pallas_call(
        functools.partial(kernel, sizes),
        out_shape=(
            jax.ShapeDtypeStruct((1, periods), f32),
            jax.ShapeDtypeStruct((1, periods), f32),
            jax.ShapeDtypeStruct((local_types, 2, periods), f32),
        ),
        in_specs=[far, smem, far, smem, smem, smem, smem, smem, vmem, vmem, vmem, smem],
        out_specs=(vmem, vmem, vmem),
        scratch_shapes=[
            pltpu.VMEM((periods, mine, incomes, assets), jnp.int32),
            pltpu.VMEM((mine, incomes, assets), f32),
            per_type, per_type, per_type,
            per_period, per_period, per_period,
            pltpu.VMEM((2 * mine, periods, ROWS, LANES), f32),
            pltpu.VMEM((incomes, ROWS, LANES), f32),
            pltpu.VMEM((incomes, ROWS, LANES), f32),
            pltpu.VMEM((ROWS, LANES), f32),
            pltpu.VMEM((3, ROWS, LANES), f32),
            pltpu.VMEM((NEWTON + ROWS, 1, LANES), f32),
            pltpu.VMEM((devices + ROWS, 1, LANES), f32),
            pltpu.VMEM((devices + ROWS, 1, LANES), f32),
            pltpu.SemaphoreType.DMA((periods,)),
            pltpu.SemaphoreType.DMA((cores - 1, here)),
            pltpu.SemaphoreType.DMA((1,)),
            pltpu.SemaphoreType.DMA((NEWTON,)),
            pltpu.SemaphoreType.DMA((NEWTON,)),
        ],
        compiler_params=pltpu.CompilerParams(collective_id=0, has_side_effects=True),
    )(*args)
    price, gap, paths = pl.pallas_call(
        hand_out,
        out_shape=tuple(jax.ShapeDtypeStruct(x.shape, f32) for x in (price, gap, paths)),
        in_specs=[vmem] * 3,
        out_specs=(vmem,) * 3,
    )(price, gap, paths)
    return price.reshape(periods), gap.reshape(periods), paths


def solution(mesh):
    placed = (
        P("types", "tm", None, None),
        P("types"),
        P("types", None, None),
        P("types"),
        P("types"),
        P(),
        P(),
        P(),
        P(),
        P(),
        P(),
        P(),
    )
    return jax.shard_map(
        functools.partial(body, mesh.shape["types"], mesh.shape["tm"]),
        mesh=mesh,
        in_specs=placed,
        out_specs=(P(), P(), P("types", None, None)),
        check_vma=False,
    )
```
